32 devices in a mesh: box: 16 (over z, y, core), lev: 2 (over x).
Axes of the slice: x: 2, y: 2, z: 4, core: 2. Of those that a mesh axis runs over, the one named last changes fastest.
Arguments:
- fine: float32 [96, 5, 32, 1024], P(('box', 'lev')), may hold values from -12 to 12
- coarse: float32 [5, 256, 32, 128], P(None, 'box', 'lev'), may hold values from -6 to 6
- owner_map: int32 [96, 2], P(('box', 'lev')), may hold values from -2 to 7, as said below
- patch_count: int32 [32], P(('box', 'lev')), may hold values from 1 to 3, as said below
- face_mask: int32 [96, 6], P(('box', 'lev')), may hold values 0 or 1
Outputs:
- updated: float32 [5, 256, 32, 128], P(None, 'box', 'lev')
- ghost: float32 [96, 6, 5, 2048], P(('box', 'lev'))
The draws below stay inside these ranges and needn't reach their ends.
Inputs may be any that keep to these rules, and one draw needn't show every extreme that they name: `owner_map`: row p is fine patch p of device j = p // 3: column 0 is the offset k of its coarse owner, device (j + k) mod 32, one of -2, -1, 1, 2 and different for the 3 rows of one device; column 1 is a region r of that owner's block, 0 to 7. Rows of patches that are not live carry entries of the same kind and are ignored. No two live patches name the same owner and region. Device j holds live patches j * 3 to j * 3 + patch_count[j] - 1. Some device holds 3 live patches.
All inputs are finite; a program needn't handle non-finite values. No bound on the sum of `face_mask` on one device may be relied on, other than what follows from the above.
Results may differ from the reference program's by a relative error of at most 0.0003.
Values sent between devices are 32-bit elements; how exact they have to be, the bound alone decides.
A program may use at most 128 MiB of HBM per device.

```python
import jax
import jax.numpy as jnp
from jax import lax

FIELDS = 5
F = 32
FPD = 3
R = 8
CZ = 128
NBLOCKS = 32
NFINE = 96
NX = 256
NY = 32
N_LEV = 2


def owner_table(key):
    first_key = jax.random.fold_in(key, 101)
    second_key = jax.random.fold_in(key, 202)
    base_offsets = jnp.tile(jnp.arange(4, dtype=jnp.int32), (NBLOCKS, 1))
    ordering = jax.random.permutation(first_key, base_offsets, axis=1, independent=True)[:, :FPD]
    delta_table = jnp.array([-2, -1, 1, 2], dtype=jnp.int32)
    offsets = delta_table[ordering]
    region_base = jnp.tile(jnp.arange(R, dtype=jnp.int32), (NBLOCKS, 1))
    region_perm = jax.random.permutation(second_key, region_base, axis=1, independent=True)
    target = (jnp.arange(NBLOCKS, dtype=jnp.int32)[:, None] + offsets) % NBLOCKS
    regions = region_perm[target, ordering]
    return jnp.stack([offsets.reshape(-1), regions.reshape(-1)], axis=1).astype(jnp.int32)


def draw_owner_map(key, part):
    return owner_table(key)


def draw_patch_count(key, part):
    counts = jax.random.randint(jax.random.fold_in(key, 7), (NBLOCKS,), 1, FPD + 1)
    fullest = jax.random.randint(jax.random.fold_in(key, 9), (), 0, NBLOCKS)
    return jnp.where(jnp.arange(NBLOCKS) == fullest, FPD, counts).astype(jnp.int32)


def touch_ends(values, own_key, smallest, top_value):
    spot = [jax.random.randint(jax.random.fold_in(own_key, axis), (), 0, length) for axis, length in enumerate(values.shape)]
    longest = values.shape.index(max(values.shape))
    next_to = spot[:longest] + [(spot[longest] + 1) % values.shape[longest]] + spot[longest + 1:]
    return values.at[tuple(spot)].set(smallest).at[tuple(next_to)].set(top_value)


def level_of(key, shape, cuts, low, high):
    def one(dim, blocks):
        draws = jax.random.uniform(jax.random.fold_in(jax.random.fold_in(key, 6), dim), (blocks,), jnp.float32, low / len(cuts), high / len(cuts))
        return jnp.repeat(jnp.exp(draws), shape[dim] // blocks).reshape((-1,) + (1,) * (len(shape) - dim - 1))

    level = one(*cuts[0])
    for cut in cuts[1:]:
        level = level * one(*cut)
    return level


def centred(stream_key, dims, scale, reach, shards=(), kind=jnp.bfloat16):
    factor_of = level_of(stream_key, dims, shards, -0.22, 0.18) if shards else 1.0
    entries = jax.random.normal(stream_key, dims, jnp.float32) * scale * factor_of
    return jnp.minimum(jnp.maximum(entries, -reach), reach).astype(kind)


def setup_inputs(seed: int = 0) -> dict:
    streams_of = jax.random.split(jax.random.key(seed), 6)
    fine = centred(streams_of[0], (NFINE, FIELDS, F, F * F), 2.0, 12.0, ((0, 32),), jnp.float32)
    coarse = centred(streams_of[1], (FIELDS, NX, NY, CZ), 1.0, 6.0, ((1, 16), (2, 2)), jnp.float32)
    owner_map = draw_owner_map(jax.random.fold_in(streams_of[5], 71), 0)
    patch_count = draw_patch_count(jax.random.fold_in(streams_of[5], 71), 0)
    face_mask = touch_ends((jax.random.randint(streams_of[4], (NFINE, 6), 0, 4) < 3).astype(jnp.int32), jax.random.fold_in(streams_of[4], 1), 0, 1)
    return {"fine": fine, "coarse": coarse, "owner_map": owner_map, "patch_count": patch_count, "face_mask": face_mask}


def restrict(fine):
    coarse_edge = fine.shape[2] // 2
    grouped = fine.reshape(fine.shape[0], fine.shape[1], coarse_edge, 2, coarse_edge, 2, coarse_edge, 2)
    return jnp.sum(grouped, axis=(3, 5, 7)) * 0.125


def widen(values):
    return jnp.repeat(jnp.repeat(jnp.repeat(values, 2, axis=1), 2, axis=2), 2, axis=3)


def interpolate(window):
    edge_cells = window.shape[1] - 4
    fine_width = 2 * edge_cells
    centre = window[:, 1:-1, 1:-1, 1:-1]
    slope_x = 0.5 * (window[:, 2:, 1:-1, 1:-1] - window[:, :-2, 1:-1, 1:-1])
    slope_y = 0.5 * (window[:, 1:-1, 2:, 1:-1] - window[:, 1:-1, :-2, 1:-1])
    slope_z = 0.5 * (window[:, 1:-1, 1:-1, 2:] - window[:, 1:-1, 1:-1, :-2])
    offset_sign = jnp.tile(jnp.array([-0.25, 0.25], dtype=window.dtype), edge_cells + 2)
    fine_value = (widen(centre) + offset_sign[None, :, None, None] * widen(slope_x)
                  + offset_sign[None, None, :, None] * widen(slope_y)
                  + offset_sign[None, None, None, :] * widen(slope_z))
    middle = slice(2, fine_width + 2)
    lower_rim = slice(0, 2)
    upper_rim = slice(fine_width + 2, fine_width + 4)
    face_list = [fine_value[:, lower_rim, middle, middle], fine_value[:, upper_rim, middle, middle],
                 fine_value[:, middle, lower_rim, middle], fine_value[:, middle, upper_rim, middle],
                 fine_value[:, middle, middle, lower_rim], fine_value[:, middle, middle, upper_rim]]
    return jnp.stack([each_face.reshape(each_face.shape[0], -1) for each_face in face_list])


def reference(fine, coarse, owner_map, patch_count, face_mask):
    coarse_edge = F // 2
    patch_total = fine.shape[0]
    per_device = patch_total // NBLOCKS
    averaged = restrict(fine)
    patch_ids = jnp.arange(patch_total, dtype=jnp.int32)
    holder = patch_ids // per_device
    is_live = (patch_ids % per_device) < patch_count[holder]
    target = (holder + owner_map[:, 0]) % NBLOCKS
    starts = jnp.stack([jnp.zeros_like(target), (target // N_LEV) * coarse_edge,
                        (target % N_LEV) * coarse_edge, owner_map[:, 1] * coarse_edge], axis=1).astype(jnp.int32)
    extent = (coarse.shape[0], coarse_edge, coarse_edge, coarse_edge)

    def write_patch(position, field):
        corner = [starts[position, 0], starts[position, 1], starts[position, 2], starts[position, 3]]
        present = lax.dynamic_slice(field, corner, extent)
        placed = jnp.where(is_live[position], averaged[position], present)
        return lax.dynamic_update_slice(field, placed, corner)

    updated = lax.fori_loop(0, patch_total, write_patch, coarse)
    padded = jnp.pad(updated, ((0, 0), (2, 2), (2, 2), (2, 2)), mode="wrap")
    window_extent = (coarse.shape[0], coarse_edge + 4, coarse_edge + 4, coarse_edge + 4)

    def ghost_of(position):
        corner = [starts[position, 0], starts[position, 1], starts[position, 2], starts[position, 3]]
        window = lax.dynamic_slice(padded, corner, window_extent)
        keep_mask = (is_live[position] & (face_mask[position] > 0)).astype(coarse.dtype)
        return interpolate(window) * keep_mask[:, None, None]

    ghosts = lax.map(ghost_of, patch_ids)
    return updated, ghosts
```

```python
import functools

import jax
import jax.numpy as jnp
from jax import lax
from jax.experimental import pallas as pl
from jax.experimental.pallas import tpu as pltpu
from jax.sharding import PartitionSpec as P

DELTAS = (-2, -1, 1, 2)
LANES = 128
SUB = 8
F32 = jnp.float32
BF16 = jnp.bfloat16
MESH_ID = pl.DeviceIdType.MESH


def iota(shape, dim):
    return lax.broadcasted_iota(jnp.int32, shape, dim)


def split(values):
    high = values.astype(BF16)
    return high, (values - high.astype(F32)).astype(BF16)


def split_lanes(values):
    return jnp.concatenate(split(values), axis=1)


def times_transposed(left, right):
    return lax.dot_general(left, right, (((1,), (1,)), ((), ())), preferred_element_type=F32)


def both(table):
    return jnp.concatenate([table, table], axis=0)


def kernel(
    n_box, n_lev, slots, fields, edge,
    owner, count, mask, fine, coarse, updated, ghost,
    half_a, half_b, send1, recv1, halo_out, halo_in, corner_out, corner_in,
    planes, zrows, send3, recv3, place_table,
    s1, r1, s2, r2, s3, r3,
):
    fine_edge = 2 * edge
    block = fields * edge
    ext = edge + SUB
    z_at = 4 * ext
    d_at = 8 * ext
    c_at = d_at + 4 * edge
    rows3 = c_at + edge
    n_dev = n_box * n_lev
    box = lax.axis_index("box")
    lev = lax.axis_index("lev")
    me = box * n_lev + lev

    def shifted(by):
        other = lax.rem(me + (by + n_dev), n_dev)
        return (lax.div(other, n_lev), lax.rem(other, n_lev))

    def beside(dx, dy):
        return (lax.rem(box + (dx + n_box), n_box), lax.rem(lev + (dy + n_lev), n_lev))

    sides = (beside(-1, 0), beside(1, 0), beside(0, -1), beside(0, 1))
    corners = tuple(beside(2 * cx - 1, 2 * cy - 1) for cx in (0, 1) for cy in (0, 1))
    barrier = pltpu.get_barrier_semaphore()
    peers = [shifted(delta) for delta in DELTAS] + list(sides) + list(corners)
    for peer in peers:
        pl.semaphore_signal(barrier, inc=1, device_id=peer, device_id_type=MESH_ID)

    live_count = count[0]
    chosen = [
        [(s < live_count) & (owner[s, 0] == delta) for delta in DELTAS] for s in range(slots)
    ]
    weight = [[jnp.where(c, 1.0, 0.0).astype(F32) for c in row] for row in chosen]

    q = iota((fine_edge * fine_edge, edge * edge), 0)
    c = iota((fine_edge * fine_edge, edge * edge), 1)
    goal = (q // (2 * fine_edge)) * edge + (q % fine_edge) // 2
    table = jnp.where(goal == c, 0.125, 0.0).astype(BF16)
    frows = fields * fine_edge
    for s in range(slots):
        high, low = split(fine[s * frows:(s + 1) * frows, :])
        got = jnp.dot(high, table, preferred_element_type=F32) + jnp.dot(
            low, table, preferred_element_type=F32
        )
        half_a[s * frows:(s + 1) * frows, :] = got[:, :LANES]
        half_b[s * frows:(s + 1) * frows, :] = got[:, LANES:]
    for h, half in enumerate((half_a, half_b)):
        averaged = [
            half[pl.ds(s * frows, block, stride=2), :] + half[pl.ds(s * frows + 1, block, stride=2), :]
            for s in range(slots)
        ]
        for k in range(4):
            total = averaged[0] * weight[0][k]
            for s in range(1, slots):
                total = total + averaged[s] * weight[s][k]
            send1[k, 0:block, h * LANES:(h + 1) * LANES] = total
    for k in range(4):
        region = jnp.int32(-1)
        for s in range(slots):
            region = jnp.where(chosen[s][k], owner[s, 1], region)
        send1[k, block:block + SUB, :] = jnp.full((SUB, 2 * LANES), 1.0, F32) * region.astype(F32)

    pl.semaphore_wait(barrier, len(peers))
    first = []
    for k, delta in enumerate(DELTAS):
        copy = pltpu.make_async_remote_copy(
            src_ref=send1.at[k], dst_ref=recv1.at[k], send_sem=s1.at[k], recv_sem=r1.at[k],
            device_id=shifted(delta), device_id_type=MESH_ID,
        )
        copy.start()
        first.append(copy)

    for pair in range(4):
        row = iota((LANES, 2 * LANES), 0)
        col = iota((LANES, 2 * LANES), 1)
        hit = (row // edge == 2 * pair + col // LANES) & (row % edge == col % edge)
        place_table[pair] = both(jnp.where(hit, 1.0, 0.0).astype(BF16))
    planes[...] = jnp.zeros_like(planes)
    zrows[...] = jnp.zeros_like(zrows)
    corner_out[...] = jnp.zeros_like(corner_out)
    for k in range(4):
        send3[k * rows3 + z_at:k * rows3 + d_at, :] = jnp.zeros((4 * ext, LANES), F32)

    for copy in first:
        copy.wait_recv()

    group = (iota((1, LANES), 1) // edge).astype(F32)
    region_rows = [recv1[k, block:block + 1, 0:LANES] for k in range(4)]
    here = [group == region_rows[k] for k in range(4)]
    for h in range(2):
        stacked = split_lanes(
            jnp.concatenate([recv1[k, 0:block, h * LANES:(h + 1) * LANES] for k in range(4)], axis=0)
        )
        for pair in range(4):
            spread = jnp.dot(stacked, place_table[pair], preferred_element_type=F32)
            for odd in range(2):
                y = h * SUB + 2 * pair + odd
                merged = coarse[pl.ds(y, block, stride=edge), :]
                for k in range(4):
                    merged = jnp.where(
                        here[k], spread[k * block:(k + 1) * block, odd * LANES:(odd + 1) * LANES], merged
                    )
                updated[pl.ds(y, block, stride=edge), :] = merged
                if y < 2:
                    halo_out[2, y * block:(y + 1) * block, :] = merged
                if y >= edge - 2:
                    layer = edge - 1 - y
                    halo_out[3, layer * block:(layer + 1) * block, :] = merged
    for f in range(fields):
        for layer in range(2):
            for side, x in ((0, layer), (1, edge - 1 - layer)):
                at = f * edge * edge + x * edge
                to = (layer * fields + f) * edge
                halo_out[side, to:to + edge, :] = updated[at:at + edge, :]
    for cx in (0, 1):
        for cy in (0, 1):
            for f in range(fields):
                at = f * edge * edge + cx * (edge - 1) * edge + cy * (edge - 1)
                corner_out[2 * cx + cy, f:f + 1, :] = updated[at:at + 1, :]

    second = []
    for side in range(4):
        copy = pltpu.make_async_remote_copy(
            src_ref=halo_out.at[side], dst_ref=halo_in.at[side ^ 1],
            send_sem=s2.at[side], recv_sem=r2.at[side ^ 1],
            device_id=sides[side], device_id_type=MESH_ID,
        )
        copy.start()
        second.append(copy)
    for corner in range(4):
        copy = pltpu.make_async_remote_copy(
            src_ref=corner_out.at[corner], dst_ref=corner_in.at[3 - corner],
            send_sem=s2.at[4 + corner], recv_sem=r2.at[4 + 3 - corner],
            device_id=corners[corner], device_id_type=MESH_ID,
        )
        copy.start()
        second.append(copy)

    lane = iota((1, LANES), 1).astype(F32)

    def pick(k, place):
        t = lane - edge * region_rows[k] - place
        return jnp.where((t == 0.0) | (t == LANES) | (t == -LANES), 1.0, 0.0)

    i_side = iota((ext, 1), 0)
    place = jnp.where(i_side == edge, -1, jnp.where(i_side == edge + 1, edge, i_side)).astype(F32)
    used = i_side < edge + 2
    side_table = jnp.concatenate(
        [jnp.where(used, pick(k, place), 0.0) for k in range(4)], axis=0
    ).astype(BF16)
    side_table = jnp.concatenate([side_table, side_table], axis=1)
    i_z = iota((SUB, 1), 0)
    plus = jnp.where(i_z == 0, -1, jnp.where(i_z == 1, 0, jnp.where(i_z == 2, edge, edge + 1)))
    minus = jnp.where(i_z == 1, -2, edge - 1)
    z_list = []
    for k in range(4):
        up = pick(k, plus.astype(F32))
        down = jnp.where((i_z == 1) | (i_z == 3), pick(k, minus.astype(F32)), 0.0)
        z_list.append(jnp.where(i_z < 4, up - down, 0.0))
    z_table = jnp.concatenate(z_list, axis=0).astype(BF16)
    z_table = jnp.concatenate([z_table, z_table], axis=1)

    def z_store(v, values):
        for k in range(4):
            send3[pl.ds(k * rows3 + z_at + v, 4, stride=ext), :] = values[k * SUB:k * SUB + 4, :]

    for v in range(edge):
        for f in range(fields):
            zrows[pl.ds(v * LANES + f, edge, stride=SUB), :] = updated[
                pl.ds(f * edge * edge + v, edge, stride=edge), :
            ]
    for v in range(0, edge, 2):
        got = times_transposed(z_table, split_lanes(zrows[v * LANES:(v + 2) * LANES, :]))
        z_store(v, got[:, :LANES])
        z_store(v + 1, got[:, LANES:])

    def line_tables(cell, odd):
        i = iota((ext, LANES), 0)
        at = jnp.where(i == edge, -1, jnp.where(i == edge + 1, edge, i))
        at = jnp.where(i < edge + 2, at, -9)
        plain = jnp.where(at == cell, 1.0, 0.0)
        sign = jnp.where(odd, 0.125, -0.125)
        slope = jnp.where(at == cell + 1, sign, jnp.where(at == cell - 1, -sign, 0.0))
        full = both(jnp.concatenate([plain, plain + slope], axis=1)).astype(BF16)
        return full, both((plain[:edge] * 0.125)).astype(BF16)

    l2 = iota((ext, LANES), 1)
    w_table, w_diff = line_tables((l2 % fine_edge) // 2, l2 % 2 == 1)
    v_table, v_diff = line_tables((l2 % (2 * fine_edge)) // 4, (l2 // 2) % 2 == 1)
    row = iota((LANES, LANES), 0)
    col = iota((LANES, LANES), 1)
    line_v = both(jnp.where(row // SUB == (col % (2 * fine_edge)) // 4, 1.0, 0.0).astype(BF16))

    for copy in second:
        copy.wait_recv()

    for side in range(4):
        near = 1.0 if side % 2 == 0 else -1.0
        for f in range(fields):
            a = f * edge
            adjacent = halo_in[side, a:a + edge, :]
            far = halo_in[side, block + a:block + a + edge, :]
            own = halo_out[side, a:a + edge, :]
            planes[pl.ds(2 * side * LANES + f, edge, stride=SUB), :] = adjacent
            planes[pl.ds((2 * side + 1) * LANES + f, edge, stride=SUB), :] = (own - far) * near
    for corner in range(4):
        planes[8 * LANES + corner * SUB:8 * LANES + (corner + 1) * SUB, :] = corner_in[corner]
    for side in range(4):
        both_planes = split_lanes(planes[2 * side * LANES:(2 * side + 2) * LANES, :])
        got = times_transposed(side_table, both_planes)
        for k in range(4):
            at = k * rows3
            send3[at + side * ext:at + (side + 1) * ext, :] = got[k * ext:(k + 1) * ext, :LANES]
            to = at + d_at + side * edge
            send3[to:to + edge, :] = got[k * ext:k * ext + edge, LANES:]
        if side >= 2:
            z_store(edge + side - 2, times_transposed(z_table, both_planes[:LANES, :]))
    got = times_transposed(side_table, split_lanes(planes[8 * LANES:9 * LANES, :]))
    for k in range(4):
        send3[k * rows3 + c_at:k * rows3 + c_at + edge, :] = got[k * ext:k * ext + edge, :]

    third = []
    for k, delta in enumerate(DELTAS):
        copy = pltpu.make_async_remote_copy(
            src_ref=send3.at[pl.ds(k * rows3, rows3)], dst_ref=recv3.at[k],
            send_sem=s3.at[k], recv_sem=r3.at[k],
            device_id=shifted(-delta), device_id_type=MESH_ID,
        )
        copy.start()
        third.append(copy)
    for copy in third:
        copy.wait_recv()

    lanes8 = iota((SUB, LANES), 1)
    low_half = lanes8 < 2 * fine_edge
    half_sign = jnp.where(low_half, -0.125, 0.125)
    quarter = (lanes8 // fine_edge) % 2 == 1
    quarter_slope = jnp.where(quarter, 0.125, -0.125)
    quarter_sign = jnp.where(quarter, 1.0, -1.0)
    last_sign = jnp.where(lanes8 % 2 == 1, 1.0, -1.0)
    own_field = lanes8 % SUB == iota((SUB, LANES), 0)

    def spread_plane(s, at, length, table):
        total = recv3[0, at:at + length, :] * weight[s][0]
        for k in range(1, 4):
            total = total + recv3[k, at:at + length, :] * weight[s][k]
        high = total.astype(BF16).astype(F32)
        tall = jnp.concatenate([high, total - high], axis=0)
        return total, jnp.dot(tall.T.astype(BF16), table, preferred_element_type=F32)

    def cut(values, m):
        return values[m * SUB:(m + 1) * SUB, :]

    for s in range(slots):
        keep = [
            jnp.where((s < live_count) & (mask[s, face] > 0), 1.0, 0.0).astype(F32)
            for face in range(6)
        ]
        _, lines = spread_plane(s, c_at, edge, w_diff)
        line = [cut(lines, corner) * 8.0 for corner in range(4)]
        edges = []
        for side in range(4):
            raw, centre = spread_plane(s, side * ext, ext, w_table)
            _, diff = spread_plane(s, d_at + side * edge, edge, w_diff)
            plain = [cut(centre, m)[:, :LANES] for m in range(edge)]
            full = [cut(centre, m)[:, LANES:] for m in range(edge)]
            high_side = side % 2
            if side < 2:
                edges.append(raw[edge:edge + 1, :])
                edges.append(raw[edge + 1:edge + 2, :])
                around = [line[2 * high_side]] + plain + [line[2 * high_side + 1]]
                for t in range(edge // 2):
                    base = jnp.where(low_half, full[2 * t], full[2 * t + 1])
                    slope = jnp.where(
                        low_half, around[2 * t + 2] - around[2 * t], around[2 * t + 3] - around[2 * t + 1]
                    )
                    across = jnp.where(low_half, cut(diff, 2 * t), cut(diff, 2 * t + 1))
                    base = base + slope * quarter_slope
                    at = t * LANES
                    ghost[s, side, :, at:at + LANES] = ((base - across) * keep[side])[:fields]
                    at = at + fine_edge * fine_edge
                    ghost[s, side, :, at:at + LANES] = ((base + across) * keep[side])[:fields]
            else:
                around = [line[high_side]] + plain + [line[2 + high_side]]
                for t in range(edge):
                    value = (
                        full[t] + (around[t + 2] - around[t]) * half_sign + cut(diff, t) * quarter_sign
                    )
                    ghost[s, side, :, t * LANES:(t + 1) * LANES] = (value * keep[side])[:fields]
        tall = jnp.concatenate([jnp.where(own_field, e, 0.0) for e in edges], axis=0)
        ends = jnp.dot(split_lanes(tall), line_v, preferred_element_type=F32)
        for z in range(2):
            _, centre = spread_plane(s, z_at + 2 * z * ext, ext, v_table)
            _, diff = spread_plane(s, z_at + (2 * z + 1) * ext, edge, v_diff)
            around = (
                [cut(ends, z)] + [cut(centre, m)[:, :LANES] for m in range(edge)] + [cut(ends, 2 + z)]
            )
            for t in range(edge):
                value = (
                    cut(centre, t)[:, LANES:]
                    + (around[t + 2] - around[t]) * half_sign
                    + cut(diff, t) * last_sign
                )
                ghost[s, 4 + z, :, t * LANES:(t + 1) * LANES] = (value * keep[4 + z])[:fields]

    for copy in first + second + third:
        copy.wait_send()


def body(n_box, n_lev, fine, coarse, owner_map, patch_count, face_mask):
    slots, fields, fine_edge, _ = fine.shape
    edge = fine_edge // 2
    block = fields * edge
    ext = edge + SUB
    rows3 = 8 * ext + 5 * edge
    vmem = pl.BlockSpec(memory_space=pltpu.VMEM)
    smem = pl.BlockSpec(memory_space=pltpu.SMEM)
    updated, ghost = pl.pallas_call(
        functools.partial(kernel, n_box, n_lev, slots, fields, edge),
        out_shape=(
            jax.ShapeDtypeStruct((block * edge, LANES), F32),
            jax.ShapeDtypeStruct((slots, 6, fields, 2 * fine_edge * fine_edge), F32),
        ),
        in_specs=[smem, smem, smem, vmem, vmem],
        out_specs=(vmem, vmem),
        scratch_shapes=[
            pltpu.VMEM((slots * fields * fine_edge, LANES), F32),
            pltpu.VMEM((slots * fields * fine_edge, LANES), F32),
            pltpu.VMEM((4, block + SUB, 2 * LANES), F32),
            pltpu.VMEM((4, block + SUB, 2 * LANES), F32),
            pltpu.VMEM((4, 2 * block, LANES), F32),
            pltpu.VMEM((4, 2 * block, LANES), F32),
            pltpu.VMEM((4, SUB, LANES), F32),
            pltpu.VMEM((4, SUB, LANES), F32),
            pltpu.VMEM((9 * LANES, LANES), F32),
            pltpu.VMEM((edge * LANES, LANES), F32),
            pltpu.VMEM((4 * rows3, LANES), F32),
            pltpu.VMEM((4, rows3, LANES), F32),
            pltpu.VMEM((4, 2 * LANES, 2 * LANES), BF16),
            pltpu.SemaphoreType.DMA((4,)),
            pltpu.SemaphoreType.DMA((4,)),
            pltpu.SemaphoreType.DMA((8,)),
            pltpu.SemaphoreType.DMA((8,)),
            pltpu.SemaphoreType.DMA((4,)),
            pltpu.SemaphoreType.DMA((4,)),
        ],
        compiler_params=pltpu.CompilerParams(collective_id=0, has_side_effects=True),
    )(
        owner_map, patch_count, face_mask,
        fine.reshape(slots * fields * fine_edge, fine_edge * fine_edge),
        coarse.reshape(block * edge, LANES),
    )
    return updated.reshape(coarse.shape), ghost


def solution(mesh):
    return jax.shard_map(
        functools.partial(body, mesh.shape["box"], mesh.shape["lev"]),
        mesh=mesh,
        in_specs=(
            P(("box", "lev"), None, None, None),
            P(None, "box", "lev", None),
            P(("box", "lev"), None),
            P(("box", "lev")),
            P(("box", "lev"), None),
        ),
        out_specs=(P(None, "box", "lev", None), P(("box", "lev"), None, None, None)),
        check_vma=False,
    )
```

```python
import functools

import jax
import jax.numpy as jnp
from jax import lax
from jax.experimental import pallas as pl
from jax.experimental.pallas import tpu as pltpu
from jax.sharding import PartitionSpec as P

DELTAS = (-2, -1, 1, 2)
LANES = 128
SUB = 8
F32 = jnp.float32
BF16 = jnp.bfloat16
MESH_ID = pl.DeviceIdType.MESH


def iota(shape, dim):
    return lax.broadcasted_iota(jnp.int32, shape, dim)


def split(values):
    high = values.astype(BF16)
    return high, (values - high.astype(F32)).astype(BF16)


def split_lanes(values):
    return jnp.concatenate(split(values), axis=1)


def times_transposed(left, right):
    return lax.dot_general(left, right, (((1,), (1,)), ((), ())), preferred_element_type=F32)


def both(table):
    return jnp.concatenate([table, table], axis=0)


def window_rows(edge):
    z_at = 4 * edge
    d_at = 6 * edge
    return 14 * edge, z_at, d_at, d_at + 4 * edge, d_at + 6 * edge, d_at + 7 * edge


def kernel(
    n_box, n_lev, slots, fields, edge,
    owner, count, fine_far, coarse_far, updated, window,
    fine, coarse, half_a, half_b, send1, recv1, halo_out, halo_in, corner_out, corner_in,
    planes, zrows, send3, recv3, place_table,
    load, s1, r1, s2, r2, s3, r3,
):
    fine_edge = 2 * edge
    block = fields * edge
    ext = edge + SUB
    rows3, z_at, d_at, zd_at, c_at, e_at = window_rows(edge)
    frows = fields * fine_edge
    cut = (fields + 1) // 2
    chunks = ((0, cut), (cut, fields))
    loads = {}
    for part, (f0, f1) in enumerate(chunks):
        for s in range(slots):
            rows = pl.ds(s * frows + f0 * fine_edge, (f1 - f0) * fine_edge)
            loads[part, s] = pltpu.make_async_copy(
                fine_far.at[rows], fine.at[rows], load.at[part * slots + s]
            )
            loads[part, s].start()
    coarse_load = pltpu.make_async_copy(coarse_far, coarse, load.at[2 * slots])
    coarse_load.start()
    n_dev = n_box * n_lev
    box = lax.axis_index("box")
    lev = lax.axis_index("lev")
    me = box * n_lev + lev

    def shifted(by):
        other = lax.rem(me + (by + n_dev), n_dev)
        return (lax.div(other, n_lev), lax.rem(other, n_lev))

    def beside(dx, dy):
        return (lax.rem(box + (dx + n_box), n_box), lax.rem(lev + (dy + n_lev), n_lev))

    sides = (beside(-1, 0), beside(1, 0), beside(0, -1), beside(0, 1))
    corners = tuple(beside(2 * cx - 1, 2 * cy - 1) for cx in (0, 1) for cy in (0, 1))
    barrier = pltpu.get_barrier_semaphore()
    peers = [shifted(delta) for delta in DELTAS] + list(sides) + list(corners)
    for peer in peers:
        pl.semaphore_signal(barrier, inc=1, device_id=peer, device_id_type=MESH_ID)

    live_count = count[0]
    chosen = [
        [(s < live_count) & (owner[0, s] == delta) for delta in DELTAS] for s in range(slots)
    ]
    weight = [[jnp.where(c, 1.0, 0.0).astype(F32) for c in row] for row in chosen]

    q = iota((fine_edge * fine_edge, edge * edge), 0)
    c = iota((fine_edge * fine_edge, edge * edge), 1)
    goal = (q // (2 * fine_edge)) * edge + (q % fine_edge) // 2
    table = jnp.where(goal == c, 0.125, 0.0).astype(BF16)
    for k in range(4):
        region = jnp.int32(-1)
        for s in range(slots):
            region = jnp.where(chosen[s][k], owner[1, s], region)
        send1[k, 0:SUB, :] = jnp.full((SUB, 2 * LANES), 1.0, F32) * region.astype(F32)
    first = []
    for part, (f0, f1) in enumerate(chunks):
        size = (f1 - f0) * edge
        for s in range(slots):
            loads[part, s].wait()
            rows = slice(s * frows + f0 * fine_edge, s * frows + f1 * fine_edge)
            high, low = split(fine[rows, :])
            got = jnp.dot(high, table, preferred_element_type=F32) + jnp.dot(
                low, table, preferred_element_type=F32
            )
            half_a[rows, :] = got[:, :LANES]
            half_b[rows, :] = got[:, LANES:]
        for h, half in enumerate((half_a, half_b)):
            averaged = []
            for s in range(slots):
                at = s * frows + f0 * fine_edge
                averaged.append(
                    half[pl.ds(at, size, stride=2), :] + half[pl.ds(at + 1, size, stride=2), :]
                )
            for k in range(4):
                total = averaged[0] * weight[0][k]
                for s in range(1, slots):
                    total = total + averaged[s] * weight[s][k]
                at = SUB + f0 * edge
                send1[k, at:at + size, h * LANES:(h + 1) * LANES] = total
        if part == 0:
            pl.semaphore_wait(barrier, len(peers))
        start = 0 if part == 0 else SUB + f0 * edge
        rows = pl.ds(start, SUB + f1 * edge - start)
        for k, delta in enumerate(DELTAS):
            copy = pltpu.make_async_remote_copy(
                src_ref=send1.at[k, rows], dst_ref=recv1.at[k, rows],
                send_sem=s1.at[part * 4 + k], recv_sem=r1.at[part * 4 + k],
                device_id=shifted(delta), device_id_type=MESH_ID,
            )
            copy.start()
            first.append(copy)

    for pair in range(4):
        row = iota((LANES, 2 * LANES), 0)
        col = iota((LANES, 2 * LANES), 1)
        hit = (row // edge == 2 * pair + col // LANES) & (row % edge == col % edge)
        place_table[pair] = both(jnp.where(hit, 1.0, 0.0).astype(BF16))
    planes[...] = jnp.zeros_like(planes)
    zrows[...] = jnp.zeros_like(zrows)
    corner_out[...] = jnp.zeros_like(corner_out)
    for k in range(4):
        send3[k * rows3 + e_at:k * rows3 + rows3, :] = jnp.zeros((edge, LANES), F32)
    coarse_load.wait()

    group = (iota((1, LANES), 1) // edge).astype(F32)
    second = []
    for part, (f0, f1) in enumerate(chunks):
        size = (f1 - f0) * edge
        for k in range(4):
            first[part * 4 + k].wait_recv()
        if part == 0:
            region_rows = [recv1[k, 0:1, 0:LANES] for k in range(4)]
            here = [group == region_rows[k] for k in range(4)]
        at = SUB + f0 * edge
        for h in range(2):
            stacked = split_lanes(jnp.concatenate(
                [recv1[k, at:at + size, h * LANES:(h + 1) * LANES] for k in range(4)], axis=0
            ))
            for pair in range(4):
                spread = jnp.dot(stacked, place_table[pair], preferred_element_type=F32)
                for odd in range(2):
                    y = h * SUB + 2 * pair + odd
                    rows = pl.ds(f0 * edge * edge + y, size, stride=edge)
                    merged = coarse[rows, :]
                    for k in range(4):
                        merged = jnp.where(
                            here[k], spread[k * size:(k + 1) * size, odd * LANES:(odd + 1) * LANES], merged
                        )
                    updated[rows, :] = merged
                    if y < 2:
                        halo_out[2, y, f0 * edge:f1 * edge, :] = merged
                    if y >= edge - 2:
                        halo_out[3, edge - 1 - y, f0 * edge:f1 * edge, :] = merged
        for f in range(f0, f1):
            for layer in range(2):
                for side, x in ((0, layer), (1, edge - 1 - layer)):
                    at = f * edge * edge + x * edge
                    halo_out[side, layer, f * edge:(f + 1) * edge, :] = updated[at:at + edge, :]
            for cx in (0, 1):
                for cy in (0, 1):
                    at = f * edge * edge + cx * (edge - 1) * edge + cy * (edge - 1)
                    corner_out[2 * cx + cy, f:f + 1, :] = updated[at:at + 1, :]
        rows = pl.ds(f0 * edge, size)
        for side in (2, 3, 0, 1):
            copy = pltpu.make_async_remote_copy(
                src_ref=halo_out.at[side, :, rows], dst_ref=halo_in.at[side ^ 1, :, rows],
                send_sem=s2.at[part * 4 + side], recv_sem=r2.at[part * 4 + (side ^ 1)],
                device_id=sides[side], device_id_type=MESH_ID,
            )
            copy.start()
            second.append(copy)
    for corner in range(4):
        copy = pltpu.make_async_remote_copy(
            src_ref=corner_out.at[corner], dst_ref=corner_in.at[3 - corner],
            send_sem=s2.at[8 + corner], recv_sem=r2.at[8 + 3 - corner],
            device_id=corners[corner], device_id_type=MESH_ID,
        )
        copy.start()
        second.append(copy)

    lane = iota((1, LANES), 1).astype(F32)

    def pick(k, place):
        t = lane - edge * region_rows[k] - place
        return jnp.where((t == 0.0) | (t == LANES) | (t == -LANES), 1.0, 0.0)

    i_side = iota((ext, 1), 0)
    place = jnp.where(i_side == edge, -1, jnp.where(i_side == edge + 1, edge, i_side)).astype(F32)
    used = i_side < edge + 2
    side_table = jnp.concatenate(
        [jnp.where(used, pick(k, place), 0.0) for k in range(4)], axis=0
    ).astype(BF16)
    side_table = jnp.concatenate([side_table, side_table], axis=1)
    i_z = iota((SUB, 1), 0)
    plus = jnp.where(i_z == 0, -1, jnp.where(i_z == 2, 0, jnp.where(i_z == 1, edge, edge + 1)))
    minus = jnp.where(i_z == 2, -2, edge - 1)
    z_list = []
    for k in range(4):
        up = pick(k, plus.astype(F32))
        down = jnp.where((i_z == 2) | (i_z == 3), pick(k, minus.astype(F32)), 0.0)
        z_list.append(jnp.where(i_z < 4, up - down, 0.0))
    z_table = jnp.concatenate(z_list, axis=0).astype(BF16)
    z_table = jnp.concatenate([z_table, z_table], axis=1)

    def z_store(v, values):
        for k in range(4):
            at = k * rows3
            level = values[k * SUB:k * SUB + 2, :]
            if v < edge:
                send3[pl.ds(at + z_at + v, 2, stride=edge), :] = level
                send3[pl.ds(at + zd_at + v, 2, stride=edge), :] = values[k * SUB + 2:k * SUB + 4, :]
            else:
                send3[pl.ds(at + e_at + 8 + v - edge, 2, stride=2), :] = level

    for v in range(edge):
        for f in range(fields):
            zrows[pl.ds(v * LANES + f, edge, stride=SUB), :] = updated[
                pl.ds(f * edge * edge + v, edge, stride=edge), :
            ]
    for v in range(0, edge, 2):
        got = times_transposed(z_table, split_lanes(zrows[v * LANES:(v + 2) * LANES, :]))
        z_store(v, got[:, :LANES])
        z_store(v + 1, got[:, LANES:])

    for copy in second:
        copy.wait_recv()

    for side in range(4):
        near = 1.0 if side % 2 == 0 else -1.0
        for f in range(fields):
            a = f * edge
            adjacent = halo_in[side, 0, a:a + edge, :]
            far = halo_in[side, 1, a:a + edge, :]
            own = halo_out[side, 0, a:a + edge, :]
            planes[pl.ds(2 * side * LANES + f, edge, stride=SUB), :] = adjacent
            planes[pl.ds((2 * side + 1) * LANES + f, edge, stride=SUB), :] = (own - far) * near
    for corner in range(4):
        planes[8 * LANES + corner * SUB:8 * LANES + (corner + 1) * SUB, :] = corner_in[corner]
    for side in range(4):
        both_planes = split_lanes(planes[2 * side * LANES:(2 * side + 2) * LANES, :])
        got = times_transposed(side_table, both_planes)
        for k in range(4):
            at = k * rows3
            send3[at + side * edge:at + (side + 1) * edge, :] = got[k * ext:k * ext + edge, :LANES]
            send3[at + e_at + 2 * side:at + e_at + 2 * side + 2, :] = (
                got[k * ext + edge:k * ext + edge + 2, :LANES]
            )
            to = at + d_at + side * edge
            send3[to:to + edge, :] = got[k * ext:k * ext + edge, LANES:]
        if side >= 2:
            z_store(edge + side - 2, times_transposed(z_table, both_planes[:LANES, :]))
    got = times_transposed(side_table, split_lanes(planes[8 * LANES:9 * LANES, :]))
    for k in range(4):
        send3[k * rows3 + c_at:k * rows3 + c_at + edge, :] = got[k * ext:k * ext + edge, :]

    third = []
    for k, delta in enumerate(DELTAS):
        copy = pltpu.make_async_remote_copy(
            src_ref=send3.at[pl.ds(k * rows3, rows3)], dst_ref=recv3.at[k],
            send_sem=s3.at[k], recv_sem=r3.at[k],
            device_id=shifted(-delta), device_id_type=MESH_ID,
        )
        copy.start()
        third.append(copy)
    for copy in third:
        copy.wait_recv()

    for s in range(slots):
        total = recv3[0] * weight[s][0]
        for k in range(1, 4):
            total = total + recv3[k] * weight[s][k]
        window[s] = total

    for copy in first + second + third:
        copy.wait_send()


def ghost_kernel(
    slots, fields, edge, count, mask, window, updated_in, updated_out, ghost_out,
    passing, ghost, pass_sem, out_sem,
):
    fine_edge = 2 * edge
    rows3, z_at, d_at, zd_at, c_at, e_at = window_rows(edge)
    live_count = count[0]
    into = pltpu.make_async_copy(updated_in, passing, pass_sem.at[0])
    into.start()

    def line_tables(cell, odd, pair):
        i = iota((2 * edge, LANES), 0)
        at = jnp.where(i == edge + pair, -1, jnp.where(i == edge + pair + 1, edge, i))
        at = jnp.where((i < edge) | (at != i), at, -9)
        plain = jnp.where(at == cell, 1.0, 0.0)
        sign = jnp.where(odd, 0.125, -0.125)
        slope = jnp.where(at == cell + 1, sign, jnp.where(at == cell - 1, -sign, 0.0))
        full = both(jnp.concatenate([plain, plain + slope], axis=1)).astype(BF16)
        return full, both((plain[:edge] * 0.125)).astype(BF16)

    l2 = iota((2 * edge, LANES), 1)
    side_tables = []
    for side in range(4):
        full, w_diff = line_tables((l2 % fine_edge) // 2, l2 % 2 == 1, 2 * side)
        side_tables.append(full)
    z_tables = []
    for z in range(2):
        full, v_diff = line_tables(
            (l2 % (2 * fine_edge)) // 4, (l2 // 2) % 2 == 1, 8 + 2 * z
        )
        z_tables.append(full)
    row = iota((LANES, LANES), 0)
    col = iota((LANES, LANES), 1)
    line_v = both(jnp.where(row // SUB == (col % (2 * fine_edge)) // 4, 1.0, 0.0).astype(BF16))

    lanes8 = iota((SUB, LANES), 1)
    low_half = lanes8 < 2 * fine_edge
    half_sign = jnp.where(low_half, -0.125, 0.125)
    quarter = (lanes8 // fine_edge) % 2 == 1
    quarter_slope = jnp.where(quarter, 0.125, -0.125)
    quarter_sign = jnp.where(quarter, 1.0, -1.0)
    last_sign = jnp.where(lanes8 % 2 == 1, 1.0, -1.0)
    own_field = lanes8 % SUB == iota((SUB, LANES), 0)

    def spread_plane(s, at, table, ends=None):
        total = window[s, at:at + edge, :]
        if ends is not None:
            total = jnp.concatenate([total, ends], axis=0)
        high = total.astype(BF16).astype(F32)
        tall = jnp.concatenate([high, total - high], axis=0)
        return jnp.dot(tall.T.astype(BF16), table, preferred_element_type=F32)

    def cut(values, m):
        return values[m * SUB:(m + 1) * SUB, :]

    outs = []
    for s in range(slots):
        keep = [
            jnp.where((s < live_count) & (mask[s, face] > 0), 1.0, 0.0).astype(F32)
            for face in range(6)
        ]
        ends_all = window[s, e_at:e_at + edge, :]
        lines = spread_plane(s, c_at, w_diff)
        line = [cut(lines, corner) * 8.0 for corner in range(4)]
        edges = []
        for side in range(4):
            centre = spread_plane(s, side * edge, side_tables[side], ends_all)
            diff = spread_plane(s, d_at + side * edge, w_diff)
            plain = [cut(centre, m)[:, :LANES] for m in range(edge)]
            full = [cut(centre, m)[:, LANES:] for m in range(edge)]
            high_side = side % 2
            if side < 2:
                edges.append(ends_all[2 * side:2 * side + 1, :])
                edges.append(ends_all[2 * side + 1:2 * side + 2, :])
                around = [line[2 * high_side]] + plain + [line[2 * high_side + 1]]
                for t in range(edge // 2):
                    base = jnp.where(low_half, full[2 * t], full[2 * t + 1])
                    slope = jnp.where(
                        low_half, around[2 * t + 2] - around[2 * t], around[2 * t + 3] - around[2 * t + 1]
                    )
                    across = jnp.where(low_half, cut(diff, 2 * t), cut(diff, 2 * t + 1))
                    base = base + slope * quarter_slope
                    at = t * LANES
                    ghost[s, :, side, at:at + LANES] = ((base - across) * keep[side])[:fields]
                    at = at + fine_edge * fine_edge
                    ghost[s, :, side, at:at + LANES] = ((base + across) * keep[side])[:fields]
            else:
                around = [line[high_side]] + plain + [line[2 + high_side]]
                for t in range(edge):
                    value = (
                        full[t] + (around[t + 2] - around[t]) * half_sign + cut(diff, t) * quarter_sign
                    )
                    ghost[s, :, side, t * LANES:(t + 1) * LANES] = (value * keep[side])[:fields]
        tall = jnp.concatenate([jnp.where(own_field, e, 0.0) for e in edges], axis=0)
        ends = jnp.dot(split_lanes(tall), line_v, preferred_element_type=F32)
        for z in range(2):
            centre = spread_plane(s, z_at + z * edge, z_tables[z], ends_all)
            diff = spread_plane(s, zd_at + z * edge, v_diff)
            around = (
                [cut(ends, z)] + [cut(centre, m)[:, :LANES] for m in range(edge)] + [cut(ends, 2 + z)]
            )
            for t in range(edge):
                value = (
                    cut(centre, t)[:, LANES:]
                    + (around[t + 2] - around[t]) * half_sign
                    + cut(diff, t) * last_sign
                )
                ghost[s, :, 4 + z, t * LANES:(t + 1) * LANES] = (value * keep[4 + z])[:fields]
        outs.append(pltpu.make_async_copy(ghost.at[s], ghost_out.at[s], out_sem.at[s]))
        outs[-1].start()
        if s == 0:
            into.wait()
            outs.append(pltpu.make_async_copy(passing, updated_out, pass_sem.at[1]))
            outs[-1].start()
    for copy in outs:
        copy.wait()


def body(n_box, n_lev, fine, coarse, owner_map, patch_count, face_mask):
    slots, fields, fine_edge, _ = fine.shape
    edge = fine_edge // 2
    block = fields * edge
    rows3 = window_rows(edge)[0]
    vmem = pl.BlockSpec(memory_space=pltpu.VMEM)
    smem = pl.BlockSpec(memory_space=pltpu.SMEM)
    far = pl.BlockSpec(memory_space=pl.ANY)
    flat = jax.ShapeDtypeStruct((block * edge, LANES), F32)
    updated, window = pl.pallas_call(
        functools.partial(kernel, n_box, n_lev, slots, fields, edge),
        out_shape=(flat, jax.ShapeDtypeStruct((slots, rows3, LANES), F32)),
        in_specs=[smem, smem, far, far],
        out_specs=(vmem, vmem),
        scratch_shapes=[
            pltpu.VMEM((slots * fields * fine_edge, fine_edge * fine_edge), F32),
            pltpu.VMEM((block * edge, LANES), F32),
            pltpu.VMEM((slots * fields * fine_edge, LANES), F32),
            pltpu.VMEM((slots * fields * fine_edge, LANES), F32),
            pltpu.VMEM((4, block + SUB, 2 * LANES), F32),
            pltpu.VMEM((4, block + SUB, 2 * LANES), F32),
            pltpu.VMEM((4, 2, block, LANES), F32),
            pltpu.VMEM((4, 2, block, LANES), F32),
            pltpu.VMEM((4, SUB, LANES), F32),
            pltpu.VMEM((4, SUB, LANES), F32),
            pltpu.VMEM((9 * LANES, LANES), F32),
            pltpu.VMEM((edge * LANES, LANES), F32),
            pltpu.VMEM((4 * rows3, LANES), F32),
            pltpu.VMEM((4, rows3, LANES), F32),
            pltpu.VMEM((4, 2 * LANES, 2 * LANES), BF16),
            pltpu.SemaphoreType.DMA((2 * slots + 1,)),
            pltpu.SemaphoreType.DMA((8,)),
            pltpu.SemaphoreType.DMA((8,)),
            pltpu.SemaphoreType.DMA((12,)),
            pltpu.SemaphoreType.DMA((12,)),
            pltpu.SemaphoreType.DMA((4,)),
            pltpu.SemaphoreType.DMA((4,)),
        ],
        compiler_params=pltpu.CompilerParams(collective_id=0, has_side_effects=True),
    )(
        owner_map.T, patch_count,
        fine.reshape(slots * fields * fine_edge, fine_edge * fine_edge),
        coarse.reshape(block * edge, LANES),
    )
    ghost_shape = (slots, fields, 6, 2 * fine_edge * fine_edge)
    updated, ghost = pl.pallas_call(
        functools.partial(ghost_kernel, slots, fields, edge),
        out_shape=(flat, jax.ShapeDtypeStruct(ghost_shape, F32)),
        in_specs=[smem, smem, vmem, far],
        out_specs=(far, far),
        scratch_shapes=[
            pltpu.VMEM((block * edge, LANES), F32),
            pltpu.VMEM(ghost_shape, F32),
            pltpu.SemaphoreType.DMA((2,)),
            pltpu.SemaphoreType.DMA((slots,)),
        ],
    )(patch_count, face_mask, window, updated)
    return updated.reshape(coarse.shape), ghost.transpose(0, 2, 1, 3)


def solution(mesh):
    return jax.shard_map(
        functools.partial(body, mesh.shape["box"], mesh.shape["lev"]),
        mesh=mesh,
        in_specs=(
            P(("box", "lev"), None, None, None),
            P(None, "box", "lev", None),
            P(("box", "lev"), None),
            P(("box", "lev")),
            P(("box", "lev"), None),
        ),
        out_specs=(P(None, "box", "lev", None), P(("box", "lev"), None, None, None)),
        check_vma=False,
    )
```

```python
import functools

import jax
import jax.numpy as jnp
from jax import lax
from jax.experimental import pallas as pl
from jax.experimental.pallas import tpu as pltpu
from jax.sharding import PartitionSpec as P

DELTAS = (-2, -1, 1, 2)
LANES = 128
SUB = 8
F32 = jnp.float32
BF16 = jnp.bfloat16
MESH_ID = pl.DeviceIdType.MESH


def iota(shape, dim):
    return lax.broadcasted_iota(jnp.int32, shape, dim)


def split(values):
    high = values.astype(BF16)
    return high, (values - high.astype(F32)).astype(BF16)


def split_lanes(values):
    return jnp.concatenate(split(values), axis=1)


def times_transposed(left, right):
    return lax.dot_general(left, right, (((1,), (1,)), ((), ())), preferred_element_type=F32)


def both(table):
    return jnp.concatenate([table, table], axis=0)


def window_rows(edge):
    return 14 * edge, 0, 8 * edge, 2 * edge, 12 * edge, 13 * edge


def kernel(
    n_box, n_lev, slots, fields, edge,
    owner, count, fine_far, coarse_far, updated, window,
    fine, coarse, half_a, half_b, send1, recv1, halo_out, halo_in, corner_out, corner_in,
    planes, zrows, send3, recv3, place_table,
    load, s1, r1, s2, r2, s3, r3,
):
    fine_edge = 2 * edge
    block = fields * edge
    ext = edge + SUB
    rows3, z_at, d_at, zd_at, c_at, e_at = window_rows(edge)
    frows = fields * fine_edge
    cut = (fields + 1) // 2
    chunks = ((0, cut), (cut, fields))
    loads = {}
    for part, (f0, f1) in enumerate(chunks):
        for s in range(slots):
            rows = pl.ds(s * frows + f0 * fine_edge, (f1 - f0) * fine_edge)
            loads[part, s] = pltpu.make_async_copy(
                fine_far.at[rows], fine.at[rows], load.at[part * slots + s]
            )
            loads[part, s].start()
    coarse_load = pltpu.make_async_copy(coarse_far, coarse, load.at[2 * slots])
    coarse_load.start()
    n_dev = n_box * n_lev
    box = lax.axis_index("box")
    lev = lax.axis_index("lev")
    me = box * n_lev + lev

    def shifted(by):
        other = lax.rem(me + (by + n_dev), n_dev)
        return (lax.div(other, n_lev), lax.rem(other, n_lev))

    def beside(dx, dy):
        return (lax.rem(box + (dx + n_box), n_box), lax.rem(lev + (dy + n_lev), n_lev))

    sides = (beside(-1, 0), beside(1, 0), beside(0, -1), beside(0, 1))
    corners = tuple(beside(2 * cx - 1, 2 * cy - 1) for cx in (0, 1) for cy in (0, 1))
    barrier = pltpu.get_barrier_semaphore()
    peers = [shifted(delta) for delta in DELTAS] + list(sides) + list(corners)
    for peer in peers:
        pl.semaphore_signal(barrier, inc=1, device_id=peer, device_id_type=MESH_ID)

    live_count = count[0]
    chosen = [
        [(s < live_count) & (owner[0, s] == delta) for delta in DELTAS] for s in range(slots)
    ]
    weight = [[jnp.where(c, 1.0, 0.0).astype(F32) for c in row] for row in chosen]

    q = iota((fine_edge * fine_edge, edge * edge), 0)
    c = iota((fine_edge * fine_edge, edge * edge), 1)
    goal = (q // (2 * fine_edge)) * edge + (q % fine_edge) // 2
    table = jnp.where(goal == c, 0.125, 0.0).astype(BF16)
    for k in range(4):
        region = jnp.int32(-1)
        for s in range(slots):
            region = jnp.where(chosen[s][k], owner[1, s], region)
        send1[k, 0:SUB, :] = jnp.full((SUB, 2 * LANES), 1.0, F32) * region.astype(F32)
    first = []
    for part, (f0, f1) in enumerate(chunks):
        size = (f1 - f0) * edge
        for s in range(slots):
            loads[part, s].wait()
            rows = slice(s * frows + f0 * fine_edge, s * frows + f1 * fine_edge)
            high, low = split(fine[rows, :])
            got = jnp.dot(high, table, preferred_element_type=F32) + jnp.dot(
                low, table, preferred_element_type=F32
            )
            half_a[rows, :] = got[:, :LANES]
            half_b[rows, :] = got[:, LANES:]
        for h, half in enumerate((half_a, half_b)):
            averaged = []
            for s in range(slots):
                at = s * frows + f0 * fine_edge
                averaged.append(
                    half[pl.ds(at, size, stride=2), :] + half[pl.ds(at + 1, size, stride=2), :]
                )
            for k in range(4):
                total = averaged[0] * weight[0][k]
                for s in range(1, slots):
                    total = total + averaged[s] * weight[s][k]
                at = SUB + f0 * edge
                send1[k, at:at + size, h * LANES:(h + 1) * LANES] = total
        if part == 0:
            pl.semaphore_wait(barrier, len(peers))
        start = 0 if part == 0 else SUB + f0 * edge
        rows = pl.ds(start, SUB + f1 * edge - start)
        for k, delta in enumerate(DELTAS):
            copy = pltpu.make_async_remote_copy(
                src_ref=send1.at[k, rows], dst_ref=recv1.at[k, rows],
                send_sem=s1.at[part * 4 + k], recv_sem=r1.at[part * 4 + k],
                device_id=shifted(delta), device_id_type=MESH_ID,
            )
            copy.start()
            first.append(copy)

    for pair in range(4):
        row = iota((LANES, 2 * LANES), 0)
        col = iota((LANES, 2 * LANES), 1)
        hit = (row // edge == 2 * pair + col // LANES) & (row % edge == col % edge)
        place_table[pair] = both(jnp.where(hit, 1.0, 0.0).astype(BF16))
    planes[...] = jnp.zeros_like(planes)
    zrows[...] = jnp.zeros_like(zrows)
    corner_out[...] = jnp.zeros_like(corner_out)
    for k in range(4):
        send3[k * rows3 + e_at:k * rows3 + rows3, :] = jnp.zeros((edge, LANES), F32)
    coarse_load.wait()

    group = (iota((1, LANES), 1) // edge).astype(F32)
    second = []
    for part, (f0, f1) in enumerate(chunks):
        size = (f1 - f0) * edge
        for k in range(4):
            first[part * 4 + k].wait_recv()
        if part == 0:
            region_rows = [recv1[k, 0:1, 0:LANES] for k in range(4)]
            here = [group == region_rows[k] for k in range(4)]
        at = SUB + f0 * edge
        for h in range(2):
            stacked = split_lanes(jnp.concatenate(
                [recv1[k, at:at + size, h * LANES:(h + 1) * LANES] for k in range(4)], axis=0
            ))
            for pair in range(4):
                spread = jnp.dot(stacked, place_table[pair], preferred_element_type=F32)
                for odd in range(2):
                    y = h * SUB + 2 * pair + odd
                    rows = pl.ds(f0 * edge * edge + y, size, stride=edge)
                    merged = coarse[rows, :]
                    for k in range(4):
                        merged = jnp.where(
                            here[k], spread[k * size:(k + 1) * size, odd * LANES:(odd + 1) * LANES], merged
                        )
                    updated[rows, :] = merged
                    if y < 2:
                        halo_out[2, y, f0 * edge:f1 * edge, :] = merged
                    if y >= edge - 2:
                        halo_out[3, edge - 1 - y, f0 * edge:f1 * edge, :] = merged
        for f in range(f0, f1):
            for layer in range(2):
                for side, x in ((0, layer), (1, edge - 1 - layer)):
                    at = f * edge * edge + x * edge
                    halo_out[side, layer, f * edge:(f + 1) * edge, :] = updated[at:at + edge, :]
            for cx in (0, 1):
                for cy in (0, 1):
                    at = f * edge * edge + cx * (edge - 1) * edge + cy * (edge - 1)
                    corner_out[2 * cx + cy, f:f + 1, :] = updated[at:at + 1, :]
        rows = pl.ds(f0 * edge, size)
        for side in (2, 3, 0, 1):
            copy = pltpu.make_async_remote_copy(
                src_ref=halo_out.at[side, :, rows], dst_ref=halo_in.at[side ^ 1, :, rows],
                send_sem=s2.at[part * 4 + side], recv_sem=r2.at[part * 4 + (side ^ 1)],
                device_id=sides[side], device_id_type=MESH_ID,
            )
            copy.start()
            second.append(copy)
    for corner in range(4):
        copy = pltpu.make_async_remote_copy(
            src_ref=corner_out.at[corner], dst_ref=corner_in.at[3 - corner],
            send_sem=s2.at[8 + corner], recv_sem=r2.at[8 + 3 - corner],
            device_id=corners[corner], device_id_type=MESH_ID,
        )
        copy.start()
        second.append(copy)

    lane = iota((1, LANES), 1).astype(F32)

    def pick(k, place):
        t = lane - edge * region_rows[k] - place
        return jnp.where((t == 0.0) | (t == LANES) | (t == -LANES), 1.0, 0.0)

    i_side = iota((ext, 1), 0)
    place = jnp.where(i_side == edge, -1, jnp.where(i_side == edge + 1, edge, i_side)).astype(F32)
    used = i_side < edge + 2
    side_table = jnp.concatenate(
        [jnp.where(used, pick(k, place), 0.0) for k in range(4)], axis=0
    ).astype(BF16)
    side_table = jnp.concatenate([side_table, side_table], axis=1)
    i_z = iota((SUB, 1), 0)
    plus = jnp.where(i_z == 0, -1, jnp.where(i_z == 2, 0, jnp.where(i_z == 1, edge, edge + 1)))
    minus = jnp.where(i_z == 2, -2, edge - 1)
    z_list = []
    for k in range(4):
        up = pick(k, plus.astype(F32))
        down = jnp.where((i_z == 2) | (i_z == 3), pick(k, minus.astype(F32)), 0.0)
        z_list.append(jnp.where(i_z < 4, up - down, 0.0))
    z_table = jnp.concatenate(z_list, axis=0).astype(BF16)
    z_table = jnp.concatenate([z_table, z_table], axis=1)

    def z_store(v, values):
        for k in range(4):
            at = k * rows3
            level = values[k * SUB:k * SUB + 2, :]
            if v < edge:
                send3[pl.ds(at + z_at + v, 2, stride=edge), :] = level
                send3[pl.ds(at + zd_at + v, 2, stride=edge), :] = values[k * SUB + 2:k * SUB + 4, :]
            else:
                send3[pl.ds(at + e_at + 8 + v - edge, 2, stride=2), :] = level

    for v in range(edge):
        for f in range(fields):
            zrows[pl.ds(v * LANES + f, edge, stride=SUB), :] = updated[
                pl.ds(f * edge * edge + v, edge, stride=edge), :
            ]
    for v in range(0, edge, 2):
        got = times_transposed(z_table, split_lanes(zrows[v * LANES:(v + 2) * LANES, :]))
        z_store(v, got[:, :LANES])
        z_store(v + 1, got[:, LANES:])

    third = []

    def send_back(part):
        start, size = ((0, 4 * edge), (4 * edge, rows3 - 4 * edge))[part]
        for k, delta in enumerate(DELTAS):
            copy = pltpu.make_async_remote_copy(
                src_ref=send3.at[pl.ds(k * rows3 + start, size)], dst_ref=recv3.at[k, pl.ds(start, size)],
                send_sem=s3.at[part * 4 + k], recv_sem=r3.at[part * 4 + k],
                device_id=shifted(-delta), device_id_type=MESH_ID,
            )
            copy.start()
            third.append(copy)

    send_back(0)
    for copy in second:
        copy.wait_recv()

    for side in range(4):
        near = 1.0 if side % 2 == 0 else -1.0
        for f in range(fields):
            a = f * edge
            adjacent = halo_in[side, 0, a:a + edge, :]
            far = halo_in[side, 1, a:a + edge, :]
            own = halo_out[side, 0, a:a + edge, :]
            planes[pl.ds(2 * side * LANES + f, edge, stride=SUB), :] = adjacent
            planes[pl.ds((2 * side + 1) * LANES + f, edge, stride=SUB), :] = (own - far) * near
    for corner in range(4):
        planes[8 * LANES + corner * SUB:8 * LANES + (corner + 1) * SUB, :] = corner_in[corner]
    for side in range(4):
        both_planes = split_lanes(planes[2 * side * LANES:(2 * side + 2) * LANES, :])
        got = times_transposed(side_table, both_planes)
        for k in range(4):
            at = k * rows3
            send3[at + (4 + side) * edge:at + (5 + side) * edge, :] = got[k * ext:k * ext + edge, :LANES]
            send3[at + e_at + 2 * side:at + e_at + 2 * side + 2, :] = (
                got[k * ext + edge:k * ext + edge + 2, :LANES]
            )
            to = at + d_at + side * edge
            send3[to:to + edge, :] = got[k * ext:k * ext + edge, LANES:]
        if side >= 2:
            z_store(edge + side - 2, times_transposed(z_table, both_planes[:LANES, :]))
    got = times_transposed(side_table, split_lanes(planes[8 * LANES:9 * LANES, :]))
    for k in range(4):
        send3[k * rows3 + c_at:k * rows3 + c_at + edge, :] = got[k * ext:k * ext + edge, :]

    send_back(1)
    for copy in third:
        copy.wait_recv()

    for s in range(slots):
        total = recv3[0] * weight[s][0]
        for k in range(1, 4):
            total = total + recv3[k] * weight[s][k]
        window[s] = total

    for copy in first + second + third:
        copy.wait_send()


def ghost_kernel(
    slots, fields, edge, count, mask, window, updated_in, updated_out, ghost_out,
    passing, ghost, pass_sem, out_sem,
):
    fine_edge = 2 * edge
    rows3, z_at, d_at, zd_at, c_at, e_at = window_rows(edge)
    live_count = count[0]
    into = pltpu.make_async_copy(updated_in, passing, pass_sem.at[0])
    into.start()

    def line_tables(cell, odd, pair):
        i = iota((2 * edge, LANES), 0)
        at = jnp.where(i == edge + pair, -1, jnp.where(i == edge + pair + 1, edge, i))
        at = jnp.where((i < edge) | (at != i), at, -9)
        plain = jnp.where(at == cell, 1.0, 0.0)
        sign = jnp.where(odd, 0.125, -0.125)
        slope = jnp.where(at == cell + 1, sign, jnp.where(at == cell - 1, -sign, 0.0))
        full = both(jnp.concatenate([plain, plain + slope], axis=1)).astype(BF16)
        return full, both((plain[:edge] * 0.125)).astype(BF16)

    l2 = iota((2 * edge, LANES), 1)
    side_tables = []
    for side in range(4):
        full, w_diff = line_tables((l2 % fine_edge) // 2, l2 % 2 == 1, 2 * side)
        side_tables.append(full)
    z_tables = []
    for z in range(2):
        full, v_diff = line_tables(
            (l2 % (2 * fine_edge)) // 4, (l2 // 2) % 2 == 1, 8 + 2 * z
        )
        z_tables.append(full)
    row = iota((LANES, LANES), 0)
    col = iota((LANES, LANES), 1)
    line_v = both(jnp.where(row // SUB == (col % (2 * fine_edge)) // 4, 1.0, 0.0).astype(BF16))

    lanes8 = iota((SUB, LANES), 1)
    low_half = lanes8 < 2 * fine_edge
    half_sign = jnp.where(low_half, -0.125, 0.125)
    quarter = (lanes8 // fine_edge) % 2 == 1
    quarter_slope = jnp.where(quarter, 0.125, -0.125)
    quarter_sign = jnp.where(quarter, 1.0, -1.0)
    last_sign = jnp.where(lanes8 % 2 == 1, 1.0, -1.0)
    own_field = lanes8 % SUB == iota((SUB, LANES), 0)

    def spread_plane(s, at, table, ends=None):
        total = window[s, at:at + edge, :]
        if ends is not None:
            total = jnp.concatenate([total, ends], axis=0)
        high = total.astype(BF16).astype(F32)
        tall = jnp.concatenate([high, total - high], axis=0)
        return jnp.dot(tall.T.astype(BF16), table, preferred_element_type=F32)

    def cut(values, m):
        return values[m * SUB:(m + 1) * SUB, :]

    outs = []
    for s in range(slots):
        keep = [
            jnp.where((s < live_count) & (mask[s, face] > 0), 1.0, 0.0).astype(F32)
            for face in range(6)
        ]
        ends_all = window[s, e_at:e_at + edge, :]
        lines = spread_plane(s, c_at, w_diff)
        line = [cut(lines, corner) * 8.0 for corner in range(4)]
        edges = []
        for side in range(4):
            centre = spread_plane(s, (4 + side) * edge, side_tables[side], ends_all)
            diff = spread_plane(s, d_at + side * edge, w_diff)
            plain = [cut(centre, m)[:, :LANES] for m in range(edge)]
            full = [cut(centre, m)[:, LANES:] for m in range(edge)]
            high_side = side % 2
            if side < 2:
                edges.append(ends_all[2 * side:2 * side + 1, :])
                edges.append(ends_all[2 * side + 1:2 * side + 2, :])
                around = [line[2 * high_side]] + plain + [line[2 * high_side + 1]]
                for t in range(edge // 2):
                    base = jnp.where(low_half, full[2 * t], full[2 * t + 1])
                    slope = jnp.where(
                        low_half, around[2 * t + 2] - around[2 * t], around[2 * t + 3] - around[2 * t + 1]
                    )
                    across = jnp.where(low_half, cut(diff, 2 * t), cut(diff, 2 * t + 1))
                    base = base + slope * quarter_slope
                    at = t * LANES
                    ghost[s, :, side, at:at + LANES] = ((base - across) * keep[side])[:fields]
                    at = at + fine_edge * fine_edge
                    ghost[s, :, side, at:at + LANES] = ((base + across) * keep[side])[:fields]
            else:
                around = [line[high_side]] + plain + [line[2 + high_side]]
                for t in range(edge):
                    value = (
                        full[t] + (around[t + 2] - around[t]) * half_sign + cut(diff, t) * quarter_sign
                    )
                    ghost[s, :, side, t * LANES:(t + 1) * LANES] = (value * keep[side])[:fields]
        tall = jnp.concatenate([jnp.where(own_field, e, 0.0) for e in edges], axis=0)
        ends = jnp.dot(split_lanes(tall), line_v, preferred_element_type=F32)
        for z in range(2):
            centre = spread_plane(s, z_at + z * edge, z_tables[z], ends_all)
            diff = spread_plane(s, zd_at + z * edge, v_diff)
            around = (
                [cut(ends, z)] + [cut(centre, m)[:, :LANES] for m in range(edge)] + [cut(ends, 2 + z)]
            )
            for t in range(edge):
                value = (
                    cut(centre, t)[:, LANES:]
                    + (around[t + 2] - around[t]) * half_sign
                    + cut(diff, t) * last_sign
                )
                ghost[s, :, 4 + z, t * LANES:(t + 1) * LANES] = (value * keep[4 + z])[:fields]
        outs.append(pltpu.make_async_copy(ghost.at[s], ghost_out.at[s], out_sem.at[s]))
        outs[-1].start()
        if s == 0:
            into.wait()
            outs.append(pltpu.make_async_copy(passing, updated_out, pass_sem.at[1]))
            outs[-1].start()
    for copy in outs:
        copy.wait()


def body(n_box, n_lev, fine, coarse, owner_map, patch_count, face_mask):
    slots, fields, fine_edge, _ = fine.shape
    edge = fine_edge // 2
    block = fields * edge
    rows3 = window_rows(edge)[0]
    vmem = pl.BlockSpec(memory_space=pltpu.VMEM)
    smem = pl.BlockSpec(memory_space=pltpu.SMEM)
    far = pl.BlockSpec(memory_space=pl.ANY)
    flat = jax.ShapeDtypeStruct((block * edge, LANES), F32)
    updated, window = pl.pallas_call(
        functools.partial(kernel, n_box, n_lev, slots, fields, edge),
        out_shape=(flat, jax.ShapeDtypeStruct((slots, rows3, LANES), F32)),
        in_specs=[smem, smem, far, far],
        out_specs=(vmem, vmem),
        scratch_shapes=[
            pltpu.VMEM((slots * fields * fine_edge, fine_edge * fine_edge), F32),
            pltpu.VMEM((block * edge, LANES), F32),
            pltpu.VMEM((slots * fields * fine_edge, LANES), F32),
            pltpu.VMEM((slots * fields * fine_edge, LANES), F32),
            pltpu.VMEM((4, block + SUB, 2 * LANES), F32),
            pltpu.VMEM((4, block + SUB, 2 * LANES), F32),
            pltpu.VMEM((4, 2, block, LANES), F32),
            pltpu.VMEM((4, 2, block, LANES), F32),
            pltpu.VMEM((4, SUB, LANES), F32),
            pltpu.VMEM((4, SUB, LANES), F32),
            pltpu.VMEM((9 * LANES, LANES), F32),
            pltpu.VMEM((edge * LANES, LANES), F32),
            pltpu.VMEM((4 * rows3, LANES), F32),
            pltpu.VMEM((4, rows3, LANES), F32),
            pltpu.VMEM((4, 2 * LANES, 2 * LANES), BF16),
            pltpu.SemaphoreType.DMA((2 * slots + 1,)),
            pltpu.SemaphoreType.DMA((8,)),
            pltpu.SemaphoreType.DMA((8,)),
            pltpu.SemaphoreType.DMA((12,)),
            pltpu.SemaphoreType.DMA((12,)),
            pltpu.SemaphoreType.DMA((8,)),
            pltpu.SemaphoreType.DMA((8,)),
        ],
        compiler_params=pltpu.CompilerParams(collective_id=0, has_side_effects=True),
    )(
        owner_map.T, patch_count,
        fine.reshape(slots * fields * fine_edge, fine_edge * fine_edge),
        coarse.reshape(block * edge, LANES),
    )
    ghost_shape = (slots, fields, 6, 2 * fine_edge * fine_edge)
    updated, ghost = pl.pallas_call(
        functools.partial(ghost_kernel, slots, fields, edge),
        out_shape=(flat, jax.ShapeDtypeStruct(ghost_shape, F32)),
        in_specs=[smem, smem, vmem, far],
        out_specs=(far, far),
        scratch_shapes=[
            pltpu.VMEM((block * edge, LANES), F32),
            pltpu.VMEM(ghost_shape, F32),
            pltpu.SemaphoreType.DMA((2,)),
            pltpu.SemaphoreType.DMA((slots,)),
        ],
    )(patch_count, face_mask, window, updated)
    return updated.reshape(coarse.shape), ghost.transpose(0, 2, 1, 3)


def solution(mesh):
    return jax.shard_map(
        functools.partial(body, mesh.shape["box"], mesh.shape["lev"]),
        mesh=mesh,
        in_specs=(
            P(("box", "lev"), None, None, None),
            P(None, "box", "lev", None),
            P(("box", "lev"), None),
            P(("box", "lev")),
            P(("box", "lev"), None),
        ),
        out_specs=(P(None, "box", "lev", None), P(("box", "lev"), None, None, None)),
        check_vma=False,
    )
```
